32 devices in a mesh: tm: 4 (over z), mem: 4 (over y, x), tile: 2 (over core).
Axes of the slice: x: 2, y: 2, z: 4, core: 2. Of those that a mesh axis runs over, the one named last changes fastest.
Arguments:
- control: float32 [40, 2, 8, 256], P('mem', None, 'tile'), may hold values from -6 to 6
- vertical_modes: float32 [64, 2], replicated, may hold values from -4 to 4
- mode_counts: int32 [8], P('tile'), may hold values from 1 to 2, as said below
- perturbations: bfloat16 [40, 8, 64, 8, 256], P('mem', 'tm', None, 'tile'), may hold values from -6 to 6
- slot_index: int32 [12], P('tm'), may hold values from 0 to 7, as said below
- blend_weight: float32 [12], P('tm'), may hold values from 0 to 1
Outputs:
- increment: float32 [12, 64, 8, 256], P('tm', None, 'tile')
The draws below stay inside these ranges and needn't reach their ends.
Inputs may be any that keep to these rules, and one draw needn't show every extreme that they name: slot_index[w] // 2 == w // 3. `mode_counts`: both ends of the range occur.
All inputs are finite; a program needn't handle non-finite values.
Results may differ from the reference program's by a relative error of at most 0.0003.
Values sent between devices are 32-bit elements; how exact they have to be, the bound alone decides.
A program may use at most 64 MiB of HBM per device.

```python
import math
import jax
import jax.numpy as jnp
from jax import lax

LEV = 64
VM = 2
SMOOTH = 4
SLOT_DEV = 2
WIN_DEV = 3
GY = 256
ENS = 40
SLOTS = 8
WIN = 12
NX = 8


def draw_slot_index(key, part):
    blocks = jnp.arange(WIN) // WIN_DEV
    offsets = jax.random.randint(key, (WIN,), 0, SLOT_DEV)
    return (blocks * SLOT_DEV + offsets).astype(jnp.int32)


def draw_mode_counts(key, part):
    first_key = jax.random.fold_in(key, 11)
    second_key = jax.random.fold_in(key, 23)
    counts = jax.random.randint(first_key, (NX,), 1, VM + 1)
    where = jax.random.randint(second_key, (), 0, NX)
    counts = counts.at[where].set(1)
    counts = counts.at[(where + 1) % NX].set(VM)
    return counts.astype(jnp.int32)


def block_scale(stream_key, dims, pieces, smallest, largest):
    gain, own = 1.0, jax.random.fold_in(stream_key, 6)
    for position, parts in pieces:
        steps = jnp.exp(jax.random.uniform(jax.random.fold_in(own, position), (parts,), jnp.float32, smallest / len(pieces), largest / len(pieces)))
        gain = gain * jnp.repeat(steps, dims[position] // parts).reshape([-1 if axis == position else 1 for axis in range(len(dims))])
    return gain


def bell_draw(rng, shape, scale, bound, pieces=(), held_as=jnp.bfloat16):
    array = scale * jax.random.normal(rng, shape, jnp.float32)
    if pieces:
        array = array * block_scale(rng, shape, pieces, -0.22, 0.18)
    return jnp.clip(array, -bound, bound).astype(held_as)


def setup_inputs(seed: int = 0) -> dict:
    splits = jax.random.split(jax.random.key(seed), 7)
    control = bell_draw(splits[0], (ENS, VM, NX, GY), 1.0, 6.0, ((0, 4), (2, 2)), jnp.float32)
    vertical_modes = bell_draw(splits[1], (LEV, VM), 1.0, 4.0, (), jnp.float32)
    mode_counts = draw_mode_counts(jax.random.fold_in(splits[6], 71), 0)
    perturbations = bell_draw(splits[3], (ENS, SLOTS, LEV, NX, GY), 1.0, 6.0, ((0, 4), (1, 4), (3, 2)))
    slot_index = draw_slot_index(jax.random.fold_in(splits[6], 71), 0)
    blend_weight = jnp.clip(1.0 * jax.random.uniform(splits[5], (WIN,), jnp.float32) ** block_scale(splits[5], (WIN,), ((0, 4),), -0.2, 0.2), 0.0, 1.0)
    return dict(control=control, vertical_modes=vertical_modes, mode_counts=mode_counts, perturbations=perturbations, slot_index=slot_index, blend_weight=blend_weight)


diffusion = 0.24

def relax_global(field):
    neighbours = jnp.roll(field, -1, axis=2) + jnp.roll(field, 1, axis=2)
    padded = jnp.pad(field, ((0, 0), (0, 0), (0, 0), (1, 1)))
    lateral = padded[:, :, :, 2:] + padded[:, :, :, :-2]
    return field + diffusion * (neighbours + lateral - 4.0 * field)

def reference(control, vertical_modes, mode_counts, perturbations, slot_index, blend_weight):
    smoothed = control
    for repeat in range(SMOOTH):
        smoothed = relax_global(smoothed)
    localized = jnp.zeros((ENS, LEV, NX, GY), jnp.float32)
    for mode_index in range(VM):
        keep_mode = (mode_index < mode_counts).astype(jnp.float32)
        masked = keep_mode[None, :, None] * smoothed[:, mode_index]
        localized = localized + vertical_modes[:, mode_index][None, :, None, None] * masked[:, None]
    norm_factor = 1.0 / math.sqrt(ENS - 1)
    slots = []
    for slot in range(SLOTS):
        member_total = lax.optimization_barrier(jnp.sum(localized * perturbations[:, slot].astype(jnp.float32), axis=0))
        slots.append(member_total * norm_factor)
    slot_increment = jnp.stack(slots)
    cumulative = jnp.cumsum(slot_increment, axis=0)
    previous = jnp.concatenate([jnp.zeros((1, LEV, NX, GY), jnp.float32), cumulative[:-1]], axis=0)
    weight = blend_weight[:, None, None, None]
    return weight * cumulative[slot_index] + (1.0 - weight) * previous[slot_index]
```

```python
import functools
import math

import jax
import jax.numpy as jnp
from jax import lax
from jax.experimental import pallas as pl
from jax.experimental.pallas import tpu as pltpu
from jax.sharding import PartitionSpec as P

SMOOTH = 4
LANES = 128
MESH = pl.DeviceIdType.MESH

diffusion = 0.24


def kernel(dims, control, perturbations, modes, counts, ext, own, near, pert, smooth, part,
           first_a, first_b, mid_a, mid_b, second_a, second_b, passing,
           load_sem, pert_sem, halo_send, halo_recv, rs_send, rs_recv, z_send, z_recv, ag_send, ag_recv):
    members, slots, modes_n, nx, halves, outer, inner, rows, tiles, steps_tm, norm = dims
    tm = lax.axis_index("tm")
    mem = lax.axis_index("mem")
    tile = lax.axis_index("tile")
    jy, ix = mem // inner, mem % inner
    level_rows = nx * halves
    part_levels = rows // level_rows

    def inner_peer(d):
        return (ix + d) % inner

    def outer_peer(d):
        return (jy + d) % outer

    def at(j, i):
        return {"mem": j * inner + i}

    load_own = pltpu.make_async_copy(control, own, load_sem)
    load_own.start()
    order = []
    for d in range(1, inner):
        order += [(0, outer_peer(e), inner_peer(d)) for e in range(1, outer + 1)]
    for e in range(1, outer):
        order += [(1, outer_peer(e), inner_peer(d)) for d in range(1, inner + 1)]
    sent = len(order)
    order += [(0, outer_peer(e), ix) for e in range(1, outer + 1)]
    order += [(1, jy, inner_peer(d)) for d in range(1, inner + 1)]
    loads = []
    for n, (p, j, i) in enumerate(order):
        copy = pltpu.make_async_copy(
            perturbations.at[:, :, j, i, p], pert.at[:, :, j, i, p], pert_sem.at[n])
        copy.start()
        loads.append(copy)

    barrier = pltpu.get_barrier_semaphore()
    tile_offsets = sorted({1 % tiles, (tiles - 1) % tiles} - {0})
    expected = len(tile_offsets) + (inner - 1) + (outer - 1)
    for d in tile_offsets:
        pl.semaphore_signal(barrier, inc=1, device_id={"tile": (tile + d) % tiles}, device_id_type=MESH)
    for d in range(1, inner):
        pl.semaphore_signal(barrier, inc=1, device_id=at(jy, inner_peer(d)), device_id_type=MESH)
    for e in range(1, outer):
        pl.semaphore_signal(barrier, inc=1, device_id=at(outer_peer(e), ix), device_id_type=MESH)

    @pl.when(tm > 0)
    def _():
        pl.semaphore_signal(barrier, inc=1, device_id={"tm": tm - 1}, device_id_type=MESH)

    @pl.when(tm < steps_tm - 1)
    def _():
        pl.semaphore_signal(barrier, inc=1, device_id={"tm": tm + 1}, device_id_type=MESH)

    chain_peers = jnp.where(tm > 0, 1, 0) + jnp.where(tm < steps_tm - 1, 1, 0)
    pl.semaphore_wait(barrier, expected + chain_peers)

    load_own.wait()
    halos = []
    for n, d in enumerate(tile_offsets):
        copy = pltpu.make_async_remote_copy(
            src_ref=own, dst_ref=near.at[n], send_sem=halo_send.at[n], recv_sem=halo_recv.at[n],
            device_id={"tile": (tile + d) % tiles}, device_id_type=MESH)
        copy.start()
        halos.append(copy)
    for copy in halos:
        copy.wait_recv()

    row = lax.broadcasted_iota(jnp.int32, (1, level_rows, LANES), 1)
    lane = lax.broadcasted_iota(jnp.int32, (1, level_rows, LANES), 2)
    lon, half = row % nx, row // nx
    first_lon, last_lon = lon == 0, lon == nx - 1
    first_lane, last_lane = lane == 0, lane == LANES - 1
    has_next, has_prev = half < halves - 1, half > 0
    back = level_rows - 1

    def relax(left, v, right):
        east = jnp.where(last_lon, pltpu.roll(right, nx - 1, 1), pltpu.roll(v, back, 1))
        west = jnp.where(first_lon, pltpu.roll(left, level_rows - (nx - 1), 1), pltpu.roll(v, 1, 1))
        up = pltpu.roll(v, LANES - 1, 2)
        up_next = jnp.where(has_next, pltpu.roll(up, level_rows - nx, 1), 0.0)
        down = pltpu.roll(v, 1, 2)
        down_next = jnp.where(has_prev, pltpu.roll(down, nx, 1), 0.0)
        lateral = jnp.where(last_lane, up_next, up) + jnp.where(first_lane, down_next, down)
        return v + diffusion * (east + west + lateral - 4.0 * v)

    count = jnp.zeros((1, level_rows, LANES), jnp.int32)
    for x in range(nx):
        count = jnp.where(lon == x, counts[x], count)

    fields = own.shape[0]
    batch = fields // 2 if fields % 2 == 0 and (fields // 2) % modes_n == 0 else fields

    def smooth_batch(b, carry):
        span = pl.ds(b * batch, batch)
        c = own[span]
        if tiles == 1:
            for _ in range(SMOOTH):
                c = relax(c, c, c)
        elif tiles == 2:
            o = near[0, span]
            for s in range(SMOOTH):
                c, o = relax(o, c, o), (relax(c, o, c) if s < SMOOTH - 1 else o)
        else:
            left, right = near[0, span], near[1, span]
            for s in range(SMOOTH):
                new = relax(left, c, right)
                if s < SMOOTH - 1:
                    left, right = relax(left, left, c), relax(c, right, right)
                c = new
        mode = lax.broadcasted_iota(jnp.int32, (batch, level_rows, LANES), 0) % modes_n
        smooth[span] = jnp.where(mode < count, c * norm, 0.0)
        return carry

    lax.fori_loop(0, fields // batch, smooth_batch, 0)

    pair = 2 * level_rows

    def block(p, j, i):
        base = ((j * inner + i) * 2 + p) * part_levels

        def body(u, carry):
            for t in range(slots):
                acc = [[None] * 2 for _ in range(modes_n)]
                for k in range(members):
                    x = pert[k, t, j, i, p, pl.ds(pl.multiple_of(u * pair, pair), pair), :].astype(jnp.float32)
                    for m in range(modes_n):
                        s = smooth[k * modes_n + m]
                        for v in range(2):
                            term = s * x[v * level_rows:(v + 1) * level_rows]
                            acc[m][v] = term if k == 0 else acc[m][v] + term
                for v in range(2):
                    total = modes[0, base + 2 * u + v] * acc[0][v]
                    for m in range(1, modes_n):
                        total = total + modes[m, base + 2 * u + v] * acc[m][v]
                    part[p, t, j, i, pl.ds(pl.multiple_of(u * pair + v * level_rows, level_rows), level_rows), :] = total
            return carry

        lax.fori_loop(0, rows // pair, body, 0)

    def remote(src, dst, send, recv, to):
        return pltpu.make_async_remote_copy(
            src_ref=src, dst_ref=dst, send_sem=send, recv_sem=recv, device_id=to, device_id_type=MESH)

    steps_in, steps_out = range(1, inner), range(1, outer)
    n_in = inner - 1
    rs1a = [remote(part.at[0, :, :, inner_peer(d)], first_a.at[d - 1],
                   rs_send.at[0, d - 1], rs_recv.at[0, d - 1], at(jy, inner_peer(d))) for d in steps_in]
    rs1b = [remote(part.at[1, :, outer_peer(e)], first_b.at[e - 1],
                   rs_send.at[1, e - 1], rs_recv.at[1, e - 1], at(outer_peer(e), ix)) for e in steps_out]
    rs2a = [remote(mid_a.at[e - 1], second_a.at[e - 1],
                   rs_send.at[2, e - 1], rs_recv.at[2, e - 1], at(outer_peer(e), ix)) for e in steps_out]
    rs2b = [remote(mid_b.at[d - 1], second_b.at[d - 1],
                   rs_send.at[3, d - 1], rs_recv.at[3, d - 1], at(jy, inner_peer(d))) for d in steps_in]

    n = 0
    for copy in rs1a:
        for _ in range(outer):
            loads[n].wait()
            block(*order[n])
            n += 1
        copy.start()
    for copy in rs1b:
        for _ in range(inner):
            loads[n].wait()
            block(*order[n])
            n += 1
        copy.start()
    while n < len(order):
        loads[n].wait()
        block(*order[n])
        n += 1

    for copy in rs1a:
        copy.wait_recv()
    for e, copy in zip(steps_out, rs2a):
        total = part[0, :, outer_peer(e), ix]
        for d in steps_in:
            total = total + first_a[d - 1, :, outer_peer(e)]
        mid_a[e - 1] = total
        copy.start()
    for copy in rs1b:
        copy.wait_recv()
    for d, copy in zip(steps_in, rs2b):
        total = part[1, :, jy, inner_peer(d)]
        for e in steps_out:
            total = total + first_b[e - 1, :, inner_peer(d)]
        mid_b[d - 1] = total
        copy.start()

    def gathers(unit, row0, p):
        sends, relays = [], []

        def move(j, i, to, sem):
            ref = ext.at[pl.ds(unit, slots) if unit else pl.ds(0, 1), j, i, p]
            return remote(ref, ref, ag_send.at[row0, p, sem], ag_recv.at[row0, p, sem], to)

        sem = 0
        for d in steps_in:
            sends.append(("in", d, move(jy, ix, at(jy, inner_peer(d)), sem)))
            sem += 1
        for e in steps_out:
            sends.append(("out", e, move(jy, ix, at(outer_peer(e), ix), sem)))
            sem += 1
        if p == 0:
            for d in steps_in:
                for e in steps_out:
                    relays.append((d, move(jy, inner_peer(inner - d), at(outer_peer(e), ix), sem)))
                    sem += 1
        else:
            for e in steps_out:
                for d in steps_in:
                    relays.append((e, move(outer_peer(outer - e), ix, at(jy, inner_peer(d)), sem)))
                    sem += 1
        return sends, relays

    slot_gathers = [gathers(1, 0, p) for p in range(2)]
    early_gathers = [gathers(0, 1, p) for p in range(2)]

    def start_gather(g):
        for _, _, copy in g[0]:
            copy.start()

    def relay_gather(g, p):
        kind = "in" if p == 0 else "out"
        for name, d, copy in g[0]:
            if name == kind:
                copy.wait_recv()
                for dd, forward in g[1]:
                    if dd == d:
                        forward.start()

    def finish_gather(g, p):
        kind = "in" if p == 0 else "out"
        for name, _, copy in g[0]:
            if name != kind:
                copy.wait_recv()
        for _, forward in g[1]:
            forward.wait_recv()
        for _, _, copy in g[0]:
            copy.wait_send()
        for _, forward in g[1]:
            forward.wait_send()

    chain = [remote(passing.at[p], ext.at[0, jy, ix, p], z_send.at[p], z_recv.at[p], {"tm": tm + 1})
             for p in range(2)]

    def add_slots(p):
        total = ext[1, jy, ix, p]
        for t in range(1, slots):
            total = total + ext[1 + t, jy, ix, p]
        return total

    def own_total(p):
        if p == 0:
            total = part[0, :, jy, ix]
            for d in steps_in:
                total = total + first_a[d - 1, :, jy]
            for copy in rs2a:
                copy.wait_recv()
            for e in steps_out:
                total = total + second_a[e - 1]
        else:
            total = part[1, :, jy, ix]
            for e in steps_out:
                total = total + first_b[e - 1, :, ix]
            for copy in rs2b:
                copy.wait_recv()
            for d in steps_in:
                total = total + second_b[d - 1]
        ext[pl.ds(1, slots), jy, ix, p] = total

    for p in range(2):
        own_total(p)

        @pl.when(tm == 0)
        def _():
            ext[0, jy, ix, p] = jnp.zeros(ext.shape[4:], jnp.float32)
            if steps_tm > 1:
                passing[p] = add_slots(p)
                chain[p].start()

        start_gather(slot_gathers[p])

    def earlier():
        for p in range(2):
            @pl.when(tm > 0)
            def _():
                chain[p].wait_recv()

                @pl.when(tm < steps_tm - 1)
                def _():
                    passing[p] = ext[0, jy, ix, p] + add_slots(p)
                    chain[p].start()

            start_gather(early_gathers[p])

    def relays():
        for p in range(2):
            relay_gather(slot_gathers[p], p)

    @pl.when(tm <= 1)
    def _():
        earlier()
        relays()

    @pl.when(tm > 1)
    def _():
        relays()
        earlier()

    for p in range(2):
        relay_gather(early_gathers[p], p)
    for p in range(2):
        finish_gather(slot_gathers[p], p)
    for p in range(2):
        finish_gather(early_gathers[p], p)

    @pl.when(tm < steps_tm - 1)
    def _():
        for p in range(2):
            chain[p].wait_send()

    for copy in halos + rs1a + rs1b + rs2a + rs2b:
        copy.wait_send()


def rows_view(x, nx, gy):
    lead = x.shape[:-2]
    x = x.reshape(lead + (nx, gy // LANES, LANES))
    x = jnp.swapaxes(x, -3, -2)
    return x


def per_device(control, vertical_modes, mode_counts, perturbations, slot_index, blend_weight):
    members, slots, levels, nx, gy = perturbations.shape
    modes_n = control.shape[1]
    halves = gy // LANES
    level_rows = nx * halves
    tiles, n_mem, steps_tm = lax.axis_size("tile"), lax.axis_size("mem"), lax.axis_size("tm")
    inner = 2 if n_mem % 2 == 0 else 1
    outer = n_mem // inner
    rows = levels // (n_mem * 2) * level_rows
    assert nx >= SMOOTH and level_rows == 8 and rows % 16 == 0
    norm = 1.0 / math.sqrt(members * n_mem - 1)
    fields = members * modes_n
    c = rows_view(control, nx, gy).reshape(fields, level_rows, LANES)
    q = rows_view(perturbations, nx, gy).reshape(members, slots, outer, inner, 2, rows, LANES)
    dims = (members, slots, modes_n, nx, halves, outer, inner, rows, tiles, steps_tm, norm)
    f32 = jnp.float32
    n_in, n_out = max(inner - 1, 1), max(outer - 1, 1)
    n_gather = max(inner - 1 + outer - 1 + (inner - 1) * (outer - 1), 1)
    dma = pltpu.SemaphoreType.DMA
    ext = pl.pallas_call(
        functools.partial(kernel, dims),
        out_shape=jax.ShapeDtypeStruct((slots + 1, outer, inner, 2, rows, LANES), f32),
        in_specs=[
            pl.BlockSpec(memory_space=pl.ANY),
            pl.BlockSpec(memory_space=pl.ANY),
            pl.BlockSpec(memory_space=pltpu.SMEM),
            pl.BlockSpec(memory_space=pltpu.SMEM),
        ],
        out_specs=pl.BlockSpec(memory_space=pltpu.VMEM),
        scratch_shapes=[
            pltpu.VMEM((fields, level_rows, LANES), f32),
            pltpu.VMEM((2, fields, level_rows, LANES), f32),
            pltpu.VMEM(q.shape, q.dtype),
            pltpu.VMEM((fields, level_rows, LANES), f32),
            pltpu.VMEM((2, slots, outer, inner, rows, LANES), f32),
            pltpu.VMEM((n_in, slots, outer, rows, LANES), f32),
            pltpu.VMEM((n_out, slots, inner, rows, LANES), f32),
            pltpu.VMEM((n_out, slots, rows, LANES), f32),
            pltpu.VMEM((n_in, slots, rows, LANES), f32),
            pltpu.VMEM((n_out, slots, rows, LANES), f32),
            pltpu.VMEM((n_in, slots, rows, LANES), f32),
            pltpu.VMEM((2, rows, LANES), f32),
            dma,
            dma((2 * n_mem,)),
            dma((2,)),
            dma((2,)),
            dma((4, max(n_in, n_out))),
            dma((4, max(n_in, n_out))),
            dma((2,)),
            dma((2,)),
            dma((2, 2, n_gather)),
            dma((2, 2, n_gather)),
        ],
        compiler_params=pltpu.CompilerParams(collective_id=0, has_side_effects=True),
    )(c, q, vertical_modes.T, mode_counts)
    ext = ext.reshape(slots + 1, levels, halves, nx, LANES)
    ext = jnp.swapaxes(ext, 2, 3).reshape(slots + 1, levels, nx, gy)
    local = slot_index - lax.axis_index("tm") * slots
    out = ext[0][None]
    for t in range(slots):
        share = jnp.where(local > t, 1.0, jnp.where(local == t, blend_weight, 0.0))
        out = out + share[:, None, None, None] * ext[1 + t][None]
    return out


def solution(mesh):
    placed = (
        P("mem", None, "tile", None),
        P(),
        P("tile"),
        P("mem", "tm", None, "tile", None),
        P("tm"),
        P("tm"),
    )
    return jax.shard_map(
        per_device,
        mesh=mesh,
        in_specs=placed,
        out_specs=P("tm", None, "tile", None),
        check_vma=False,
    )
```

```python
import functools
import math

import jax
import jax.numpy as jnp
from jax import lax
from jax.experimental import pallas as pl
from jax.experimental.pallas import tpu as pltpu
from jax.sharding import PartitionSpec as P

SMOOTH = 4
CHUNKS = 4
PIECES = 4
LANES = 128
MESH = pl.DeviceIdType.MESH

diffusion = 0.24


def kernel(dims, control, perturbations, modes, counts, ext, own, near, pert, smooth, part,
           first_a, first_b, mid_a, mid_b, second_a, second_b, passing,
           load_sem, pert_sem, halo_send, halo_recv, rs_send, rs_recv, z_send, z_recv, ag_send, ag_recv):
    members, slots, modes_n, nx, halves, outer, inner, rows, tiles, steps_tm, norm = dims
    tm = lax.axis_index("tm")
    mem = lax.axis_index("mem")
    tile = lax.axis_index("tile")
    jy, ix = mem // inner, mem % inner
    level_rows = nx * halves
    part_levels = rows // level_rows

    def inner_peer(d):
        return (ix + d) % inner

    def outer_peer(d):
        return (jy + d) % outer

    def at(j, i):
        return {"mem": j * inner + i}

    load_own = pltpu.make_async_copy(control, own, load_sem)
    load_own.start()
    order = []
    for d in range(1, inner):
        order += [(0, outer_peer(e), inner_peer(d)) for e in range(1, outer + 1)]
    for e in range(1, outer):
        order += [(1, outer_peer(e), inner_peer(d)) for d in range(1, inner + 1)]
    order += [(0, outer_peer(e), ix) for e in range(1, outer + 1)]
    order += [(1, jy, inner_peer(d)) for d in range(1, inner + 1)]
    loads = []
    for n, (o, j, i) in enumerate(order):
        span = pl.ds(o * CHUNKS, CHUNKS)
        copy = pltpu.make_async_copy(
            perturbations.at[:, :, j, i, span], pert.at[:, :, j, i, span], pert_sem.at[n])
        copy.start()
        loads.append(copy)

    barrier = pltpu.get_barrier_semaphore()
    tile_offsets = sorted({1 % tiles, (tiles - 1) % tiles} - {0})
    expected = len(tile_offsets) + (inner - 1) + (outer - 1)
    for d in tile_offsets:
        pl.semaphore_signal(barrier, inc=1, device_id={"tile": (tile + d) % tiles}, device_id_type=MESH)
    for d in range(1, inner):
        pl.semaphore_signal(barrier, inc=1, device_id=at(jy, inner_peer(d)), device_id_type=MESH)
    for e in range(1, outer):
        pl.semaphore_signal(barrier, inc=1, device_id=at(outer_peer(e), ix), device_id_type=MESH)

    @pl.when(tm > 0)
    def _():
        pl.semaphore_signal(barrier, inc=1, device_id={"tm": tm - 1}, device_id_type=MESH)

    @pl.when(tm < steps_tm - 1)
    def _():
        pl.semaphore_signal(barrier, inc=1, device_id={"tm": tm + 1}, device_id_type=MESH)

    chain_peers = jnp.where(tm > 0, 1, 0) + jnp.where(tm < steps_tm - 1, 1, 0)
    pl.semaphore_wait(barrier, expected + chain_peers)

    load_own.wait()
    halos = []
    for n, d in enumerate(tile_offsets):
        copy = pltpu.make_async_remote_copy(
            src_ref=own, dst_ref=near.at[n], send_sem=halo_send.at[n], recv_sem=halo_recv.at[n],
            device_id={"tile": (tile + d) % tiles}, device_id_type=MESH)
        copy.start()
        halos.append(copy)
    for copy in halos:
        copy.wait_recv()

    row = lax.broadcasted_iota(jnp.int32, (1, level_rows, LANES), 1)
    lane = lax.broadcasted_iota(jnp.int32, (1, level_rows, LANES), 2)
    lon, half = row % nx, row // nx
    first_lon, last_lon = lon == 0, lon == nx - 1
    first_lane, last_lane = lane == 0, lane == LANES - 1
    has_next, has_prev = half < halves - 1, half > 0
    back = level_rows - 1

    def relax(left, v, right):
        east = jnp.where(last_lon, pltpu.roll(right, nx - 1, 1), pltpu.roll(v, back, 1))
        west = jnp.where(first_lon, pltpu.roll(left, level_rows - (nx - 1), 1), pltpu.roll(v, 1, 1))
        up = pltpu.roll(v, LANES - 1, 2)
        up_next = jnp.where(has_next, pltpu.roll(up, level_rows - nx, 1), 0.0)
        down = pltpu.roll(v, 1, 2)
        down_next = jnp.where(has_prev, pltpu.roll(down, nx, 1), 0.0)
        lateral = jnp.where(last_lane, up_next, up) + jnp.where(first_lane, down_next, down)
        return v + diffusion * (east + west + lateral - 4.0 * v)

    count = jnp.zeros((1, level_rows, LANES), jnp.int32)
    for x in range(nx):
        count = jnp.where(lon == x, counts[x], count)

    fields = own.shape[0]
    batch = fields // 2 if fields % 2 == 0 and (fields // 2) % modes_n == 0 else fields

    def smooth_batch(b, carry):
        span = pl.ds(b * batch, batch)
        c = own[span]
        if tiles == 1:
            for _ in range(SMOOTH):
                c = relax(c, c, c)
        elif tiles == 2:
            o = near[0, span]
            for s in range(SMOOTH):
                c, o = relax(o, c, o), (relax(c, o, c) if s < SMOOTH - 1 else o)
        else:
            left, right = near[0, span], near[1, span]
            for s in range(SMOOTH):
                new = relax(left, c, right)
                if s < SMOOTH - 1:
                    left, right = relax(left, left, c), relax(c, right, right)
                c = new
        mode = lax.broadcasted_iota(jnp.int32, (batch, level_rows, LANES), 0) % modes_n
        smooth[span] = jnp.where(mode < count, c * norm, 0.0)
        return carry

    lax.fori_loop(0, fields // batch, smooth_batch, 0)

    pair = 2 * level_rows

    def sums(p, j, i, u):
        base = ((j * inner + i) * 2 * CHUNKS + p) * part_levels + 2 * u
        for t in range(slots):
            acc = [[None] * 2 for _ in range(modes_n)]
            for k in range(members):
                x = pert[k, t, j, i, p, pl.ds(pl.multiple_of(u * pair, pair), pair), :].astype(jnp.float32)
                for m in range(modes_n):
                    s = smooth[k * modes_n + m]
                    for v in range(2):
                        term = s * x[v * level_rows:(v + 1) * level_rows]
                        acc[m][v] = term if k == 0 else acc[m][v] + term
            for v in range(2):
                total = modes[0, base + v] * acc[0][v]
                for m in range(1, modes_n):
                    total = total + modes[m, base + v] * acc[m][v]
                part[p, t, j, i, pl.ds(pl.multiple_of(u * pair + v * level_rows, level_rows), level_rows), :] = total

    pairs = rows // pair

    def sums_over(count, place):
        def body(n, carry):
            u, n = n % pairs, n // pairs
            sums(*place(n), u)
            return carry

        lax.fori_loop(0, count * pairs, body, 0)

    def remote(src, dst, send, recv, to):
        return pltpu.make_async_remote_copy(
            src_ref=src, dst_ref=dst, send_sem=send, recv_sem=recv, device_id=to, device_id_type=MESH)

    steps_in, steps_out = range(1, inner), range(1, outer)
    rs1, rs2 = [[], []], [[], []]
    for c in range(CHUNKS):
        pa, pb = c, CHUNKS + c
        rs1[0].append([remote(part.at[pa, :, :, inner_peer(d)], first_a.at[c, d - 1],
                              rs_send.at[0, c, d - 1], rs_recv.at[0, c, d - 1], at(jy, inner_peer(d)))
                       for d in steps_in])
        rs1[1].append([remote(part.at[pb, :, outer_peer(e)], first_b.at[c, e - 1],
                              rs_send.at[1, c, e - 1], rs_recv.at[1, c, e - 1], at(outer_peer(e), ix))
                       for e in steps_out])
        rs2[0].append([remote(mid_a.at[c, e - 1], second_a.at[c, e - 1],
                              rs_send.at[2, c, e - 1], rs_recv.at[2, c, e - 1], at(outer_peer(e), ix))
                       for e in steps_out])
        rs2[1].append([remote(mid_b.at[c, d - 1], second_b.at[c, d - 1],
                              rs_send.at[3, c, d - 1], rs_recv.at[3, c, d - 1], at(jy, inner_peer(d)))
                       for d in steps_in])

    n_first = (inner - 1) * outer + (outer - 1) * inner
    for copy in loads[:n_first]:
        copy.wait()
    for c in range(CHUNKS):
        for d, copy in zip(steps_in, rs1[0][c]):
            sums_over(outer, lambda n: (c, outer_peer(n), inner_peer(d)))
            copy.start()
        for e, copy in zip(steps_out, rs1[1][c]):
            sums_over(inner, lambda n: (CHUNKS + c, outer_peer(e), inner_peer(n)))
            copy.start()
    for copy in loads[n_first:]:
        copy.wait()
    sums_over(CHUNKS * outer, lambda n: (n // outer, n % outer, ix))
    sums_over(CHUNKS * inner, lambda n: (CHUNKS + n // inner, jy, n % inner))

    for c in range(CHUNKS):
        for copy in rs1[0][c]:
            copy.wait_recv()
        for e, copy in zip(steps_out, rs2[0][c]):
            total = part[c, :, outer_peer(e), ix]
            for d in steps_in:
                total = total + first_a[c, d - 1, :, outer_peer(e)]
            mid_a[c, e - 1] = total
            copy.start()
        for copy in rs1[1][c]:
            copy.wait_recv()
        for d, copy in zip(steps_in, rs2[1][c]):
            total = part[CHUNKS + c, :, jy, inner_peer(d)]
            for e in steps_out:
                total = total + first_b[c, e - 1, :, inner_peer(d)]
            mid_b[c, d - 1] = total
            copy.start()

    def gathers(unit, row0, p):
        sends, relays = [], []

        def move(j, i, to, sem):
            ref = ext.at[pl.ds(unit, slots) if unit else pl.ds(0, 1), j, i, p]
            return remote(ref, ref, ag_send.at[row0, p, sem], ag_recv.at[row0, p, sem], to)

        sem = 0
        for d in steps_in:
            sends.append(("in", d, move(jy, ix, at(jy, inner_peer(d)), sem)))
            sem += 1
        for e in steps_out:
            sends.append(("out", e, move(jy, ix, at(outer_peer(e), ix), sem)))
            sem += 1
        if p < CHUNKS:
            for d in steps_in:
                for e in steps_out:
                    relays.append((d, move(jy, inner_peer(inner - d), at(outer_peer(e), ix), sem)))
                    sem += 1
        else:
            for e in steps_out:
                for d in steps_in:
                    relays.append((e, move(outer_peer(outer - e), ix, at(jy, inner_peer(d)), sem)))
                    sem += 1
        return sends, relays

    parts = range(2 * CHUNKS)
    turn = [o * CHUNKS + c for c in range(CHUNKS) for o in range(2)]
    slot_gathers = [gathers(1, 0, p) for p in parts]
    early_gathers = [gathers(0, 1, p) for p in parts]

    def start_gather(g):
        for _, _, copy in g[0]:
            copy.start()

    def relay_gather(g, p):
        kind = "in" if p < CHUNKS else "out"
        for name, d, copy in g[0]:
            if name == kind:
                copy.wait_recv()
                for dd, forward in g[1]:
                    if dd == d:
                        forward.start()

    def finish_gather(g, p):
        kind = "in" if p < CHUNKS else "out"
        for name, _, copy in g[0]:
            if name != kind:
                copy.wait_recv()
        for _, forward in g[1]:
            forward.wait_recv()
        for _, _, copy in g[0]:
            copy.wait_send()
        for _, forward in g[1]:
            forward.wait_send()

    chain = [remote(passing.at[p], ext.at[0, jy, ix, p], z_send.at[p], z_recv.at[p], {"tm": tm + 1})
             for p in parts]

    def add_slots(p):
        total = ext[1, jy, ix, p]
        for t in range(1, slots):
            total = total + ext[1 + t, jy, ix, p]
        return total

    def own_total(p):
        c = p % CHUNKS
        total = part[p, :, jy, ix]
        if p < CHUNKS:
            for d in steps_in:
                total = total + first_a[c, d - 1, :, jy]
            for copy in rs2[0][c]:
                copy.wait_recv()
            for e in steps_out:
                total = total + second_a[c, e - 1]
        else:
            for e in steps_out:
                total = total + first_b[c, e - 1, :, ix]
            for copy in rs2[1][c]:
                copy.wait_recv()
            for d in steps_in:
                total = total + second_b[c, d - 1]
        ext[pl.ds(1, slots), jy, ix, p] = total

    for p in turn:
        own_total(p)

        @pl.when(tm == 0)
        def _():
            ext[0, jy, ix, p] = jnp.zeros(ext.shape[4:], jnp.float32)
            if steps_tm > 1:
                passing[p] = add_slots(p)
                chain[p].start()

        start_gather(slot_gathers[p])

    def earlier(p):
        @pl.when(tm > 0)
        def _():
            chain[p].wait_recv()

            @pl.when(tm < steps_tm - 1)
            def _():
                passing[p] = ext[0, jy, ix, p] + add_slots(p)
                chain[p].start()

        start_gather(early_gathers[p])

    @pl.when(tm == 1)
    def _():
        for p in turn:
            earlier(p)
            relay_gather(slot_gathers[p], p)

    @pl.when(tm != 1)
    def _():
        for p in turn:
            relay_gather(slot_gathers[p], p)
        for p in turn:
            earlier(p)

    for p in turn:
        relay_gather(early_gathers[p], p)
    for p in turn:
        finish_gather(slot_gathers[p], p)
    for p in turn:
        finish_gather(early_gathers[p], p)

    @pl.when(tm < steps_tm - 1)
    def _():
        for p in parts:
            chain[p].wait_send()

    for copy in halos:
        copy.wait_send()
    for group in rs1 + rs2:
        for copies in group:
            for copy in copies:
                copy.wait_send()


def blend(slots, ext, index, weight, out, held, sems):
    windows, total_rows, _ = out.shape
    size = total_rows // PIECES
    local = [index[w] - lax.axis_index("tm") * slots for w in range(windows)]
    shares = [[jnp.where(local[w] > t, 1.0, jnp.where(local[w] == t, weight[w], 0.0))
               for t in range(slots)] for w in range(windows)]
    copies = []
    for n in range(PIECES):
        span = pl.ds(n * size, size)
        for w in range(windows):
            total = ext[0, span]
            for t in range(slots):
                total = total + shares[w][t] * ext[1 + t, span]
            held[w, span] = total
        copy = pltpu.make_async_copy(held.at[:, span], out.at[:, span], sems.at[n])
        copy.start()
        copies.append(copy)
    for copy in copies:
        copy.wait()


def rows_view(x, nx, gy):
    lead = x.shape[:-2]
    x = x.reshape(lead + (nx, gy // LANES, LANES))
    x = jnp.swapaxes(x, -3, -2)
    return x


def per_device(control, vertical_modes, mode_counts, perturbations, slot_index, blend_weight):
    members, slots, levels, nx, gy = perturbations.shape
    modes_n = control.shape[1]
    halves = gy // LANES
    level_rows = nx * halves
    tiles, n_mem, steps_tm = lax.axis_size("tile"), lax.axis_size("mem"), lax.axis_size("tm")
    inner = 2 if n_mem % 2 == 0 else 1
    outer = n_mem // inner
    parts = 2 * CHUNKS
    rows = levels // (n_mem * parts) * level_rows
    assert nx >= SMOOTH and level_rows == 8 and rows % 16 == 0
    norm = 1.0 / math.sqrt(members * n_mem - 1)
    fields = members * modes_n
    c = rows_view(control, nx, gy).reshape(fields, level_rows, LANES)
    q = rows_view(perturbations, nx, gy).reshape(members, slots, outer, inner, parts, rows, LANES)
    dims = (members, slots, modes_n, nx, halves, outer, inner, rows, tiles, steps_tm, norm)
    f32 = jnp.float32
    n_in, n_out = max(inner - 1, 1), max(outer - 1, 1)
    n_gather = max(inner - 1 + outer - 1 + (inner - 1) * (outer - 1), 1)
    dma = pltpu.SemaphoreType.DMA
    ext = pl.pallas_call(
        functools.partial(kernel, dims),
        out_shape=pltpu.VMEM((slots + 1, outer, inner, parts, rows, LANES), f32),
        in_specs=[
            pl.BlockSpec(memory_space=pltpu.HBM),
            pl.BlockSpec(memory_space=pltpu.HBM),
            pl.BlockSpec(memory_space=pltpu.SMEM),
            pl.BlockSpec(memory_space=pltpu.SMEM),
        ],
        out_specs=pl.BlockSpec(memory_space=pltpu.VMEM),
        scratch_shapes=[
            pltpu.VMEM((fields, level_rows, LANES), f32),
            pltpu.VMEM((2, fields, level_rows, LANES), f32),
            pltpu.VMEM(q.shape, q.dtype),
            pltpu.VMEM((fields, level_rows, LANES), f32),
            pltpu.VMEM((parts, slots, outer, inner, rows, LANES), f32),
            pltpu.VMEM((CHUNKS, n_in, slots, outer, rows, LANES), f32),
            pltpu.VMEM((CHUNKS, n_out, slots, inner, rows, LANES), f32),
            pltpu.VMEM((CHUNKS, n_out, slots, rows, LANES), f32),
            pltpu.VMEM((CHUNKS, n_in, slots, rows, LANES), f32),
            pltpu.VMEM((CHUNKS, n_out, slots, rows, LANES), f32),
            pltpu.VMEM((CHUNKS, n_in, slots, rows, LANES), f32),
            pltpu.VMEM((parts, rows, LANES), f32),
            dma,
            dma((2 * n_mem,)),
            dma((2,)),
            dma((2,)),
            dma((4, CHUNKS, max(n_in, n_out))),
            dma((4, CHUNKS, max(n_in, n_out))),
            dma((parts,)),
            dma((parts,)),
            dma((2, parts, n_gather)),
            dma((2, parts, n_gather)),
        ],
        compiler_params=pltpu.CompilerParams(
            collective_id=0, has_side_effects=True),
    )(c, q, vertical_modes.T, mode_counts)
    ext = ext.reshape(slots + 1, levels * level_rows, LANES)
    windows = slot_index.shape[0]
    out = pl.pallas_call(
        functools.partial(blend, slots),
        out_shape=jax.ShapeDtypeStruct((windows, levels * level_rows, LANES), f32),
        in_specs=[
            pl.BlockSpec(memory_space=pltpu.VMEM),
            pl.BlockSpec(memory_space=pltpu.SMEM),
            pl.BlockSpec(memory_space=pltpu.SMEM),
        ],
        out_specs=pl.BlockSpec(memory_space=pltpu.HBM),
        scratch_shapes=[pltpu.VMEM((windows, levels * level_rows, LANES), f32), dma((PIECES,))],
        compiler_params=pltpu.CompilerParams(vmem_limit_bytes=8 << 20),
    )(ext, slot_index, blend_weight)
    out = out.reshape(windows, levels, halves, nx, LANES)
    return jnp.swapaxes(out, 2, 3).reshape(windows, levels, nx, gy)


def solution(mesh):
    placed = (
        P("mem", None, "tile", None),
        P(),
        P("tile"),
        P("mem", "tm", None, "tile", None),
        P("tm"),
        P("tm"),
    )
    return jax.shard_map(
        per_device,
        mesh=mesh,
        in_specs=placed,
        out_specs=P("tm", None, "tile", None),
        check_vma=False,
    )
```

```python
import functools
import math

import jax
import jax.numpy as jnp
from jax import lax
from jax.experimental import pallas as pl
from jax.experimental.pallas import tpu as pltpu
from jax.sharding import PartitionSpec as P

SMOOTH = 4
CHUNKS = 4
DIRECT = (1,)
PIECES = 4
LANES = 128
MESH = pl.DeviceIdType.MESH

diffusion = 0.24


def kernel(dims, control, perturbations, modes, counts, ext, own, near, pert, smooth, part,
           first_a, first_b, mid_a, mid_b, second_a, second_b, passing,
           load_sem, pert_sem, halo_send, halo_recv, rs_send, rs_recv, z_send, z_recv, ag_send, ag_recv):
    members, slots, modes_n, nx, halves, outer, inner, rows, tiles, steps_tm, norm = dims
    tm = lax.axis_index("tm")
    mem = lax.axis_index("mem")
    tile = lax.axis_index("tile")
    jy, ix = mem // inner, mem % inner
    level_rows = nx * halves
    part_levels = rows // level_rows

    def inner_peer(d):
        return (ix + d) % inner

    def outer_peer(d):
        return (jy + d) % outer

    def at(j, i):
        return {"mem": j * inner + i}

    load_own = pltpu.make_async_copy(control, own, load_sem)
    load_own.start()
    order = []
    for d in range(1, inner):
        order += [(0, outer_peer(e), inner_peer(d)) for e in range(1, outer + 1)]
    for e in range(1, outer):
        order += [(1, outer_peer(e), inner_peer(d)) for d in range(1, inner + 1)]
    order += [(0, outer_peer(e), ix) for e in range(1, outer + 1)]
    order += [(1, jy, inner_peer(d)) for d in range(1, inner + 1)]
    loads = []
    for n, (o, j, i) in enumerate(order):
        span = pl.ds(o * CHUNKS, CHUNKS)
        copy = pltpu.make_async_copy(
            perturbations.at[:, :, j, i, span], pert.at[:, :, j, i, span], pert_sem.at[n])
        copy.start()
        loads.append(copy)

    barrier = pltpu.get_barrier_semaphore()
    tile_offsets = sorted({1 % tiles, (tiles - 1) % tiles} - {0})
    expected = len(tile_offsets) + inner * outer - 1
    for d in tile_offsets:
        pl.semaphore_signal(barrier, inc=1, device_id={"tile": (tile + d) % tiles}, device_id_type=MESH)
    for d in range(1, inner):
        pl.semaphore_signal(barrier, inc=1, device_id=at(jy, inner_peer(d)), device_id_type=MESH)
    for e in range(1, outer):
        for d in range(inner):
            pl.semaphore_signal(barrier, inc=1, device_id=at(outer_peer(e), inner_peer(d)), device_id_type=MESH)

    @pl.when(tm > 0)
    def _():
        pl.semaphore_signal(barrier, inc=1, device_id={"tm": tm - 1}, device_id_type=MESH)

    @pl.when(tm < steps_tm - 1)
    def _():
        pl.semaphore_signal(barrier, inc=1, device_id={"tm": tm + 1}, device_id_type=MESH)

    chain_peers = jnp.where(tm > 0, 1, 0) + jnp.where(tm < steps_tm - 1, 1, 0)
    pl.semaphore_wait(barrier, expected + chain_peers)

    load_own.wait()
    halos = []
    for n, d in enumerate(tile_offsets):
        copy = pltpu.make_async_remote_copy(
            src_ref=own, dst_ref=near.at[n], send_sem=halo_send.at[n], recv_sem=halo_recv.at[n],
            device_id={"tile": (tile + d) % tiles}, device_id_type=MESH)
        copy.start()
        halos.append(copy)
    for copy in halos:
        copy.wait_recv()

    row = lax.broadcasted_iota(jnp.int32, (1, level_rows, LANES), 1)
    lane = lax.broadcasted_iota(jnp.int32, (1, level_rows, LANES), 2)
    lon, half = row % nx, row // nx
    first_lon, last_lon = lon == 0, lon == nx - 1
    first_lane, last_lane = lane == 0, lane == LANES - 1
    has_next, has_prev = half < halves - 1, half > 0
    back = level_rows - 1

    def relax(left, v, right):
        east = jnp.where(last_lon, pltpu.roll(right, nx - 1, 1), pltpu.roll(v, back, 1))
        west = jnp.where(first_lon, pltpu.roll(left, level_rows - (nx - 1), 1), pltpu.roll(v, 1, 1))
        up = pltpu.roll(v, LANES - 1, 2)
        up_next = jnp.where(has_next, pltpu.roll(up, level_rows - nx, 1), 0.0)
        down = pltpu.roll(v, 1, 2)
        down_next = jnp.where(has_prev, pltpu.roll(down, nx, 1), 0.0)
        lateral = jnp.where(last_lane, up_next, up) + jnp.where(first_lane, down_next, down)
        return v + diffusion * (east + west + lateral - 4.0 * v)

    count = jnp.zeros((1, level_rows, LANES), jnp.int32)
    for x in range(nx):
        count = jnp.where(lon == x, counts[x], count)

    fields = own.shape[0]
    batch = fields // 2 if fields % 2 == 0 and (fields // 2) % modes_n == 0 else fields

    def smooth_batch(b, carry):
        span = pl.ds(b * batch, batch)
        c = own[span]
        if tiles == 1:
            for _ in range(SMOOTH):
                c = relax(c, c, c)
        elif tiles == 2:
            o = near[0, span]
            for s in range(SMOOTH):
                c, o = relax(o, c, o), (relax(c, o, c) if s < SMOOTH - 1 else o)
        else:
            left, right = near[0, span], near[1, span]
            for s in range(SMOOTH):
                new = relax(left, c, right)
                if s < SMOOTH - 1:
                    left, right = relax(left, left, c), relax(c, right, right)
                c = new
        mode = lax.broadcasted_iota(jnp.int32, (batch, level_rows, LANES), 0) % modes_n
        smooth[span] = jnp.where(mode < count, c * norm, 0.0)
        return carry

    lax.fori_loop(0, fields // batch, smooth_batch, 0)

    pair = 2 * level_rows

    def sums(p, j, i, u):
        base = ((j * inner + i) * 2 * CHUNKS + p) * part_levels + 2 * u
        for t in range(slots):
            acc = [[None] * 2 for _ in range(modes_n)]
            for k in range(members):
                x = pert[k, t, j, i, p, pl.ds(pl.multiple_of(u * pair, pair), pair), :].astype(jnp.float32)
                for m in range(modes_n):
                    s = smooth[k * modes_n + m]
                    for v in range(2):
                        term = s * x[v * level_rows:(v + 1) * level_rows]
                        acc[m][v] = term if k == 0 else acc[m][v] + term
            for v in range(2):
                total = modes[0, base + v] * acc[0][v]
                for m in range(1, modes_n):
                    total = total + modes[m, base + v] * acc[m][v]
                part[p, t, j, i, pl.ds(pl.multiple_of(u * pair + v * level_rows, level_rows), level_rows), :] = total

    pairs = rows // pair

    def sums_over(count, place):
        def body(n, carry):
            u, n = n % pairs, n // pairs
            sums(*place(n), u)
            return carry

        lax.fori_loop(0, count * pairs, body, 0)

    def remote(src, dst, send, recv, to):
        return pltpu.make_async_remote_copy(
            src_ref=src, dst_ref=dst, send_sem=send, recv_sem=recv, device_id=to, device_id_type=MESH)

    steps_in, steps_out = range(1, inner), range(1, outer)
    rs1, rs2 = [[], []], [[], []]
    for c in range(CHUNKS):
        pa, pb = c, CHUNKS + c
        rs1[0].append([remote(part.at[pa, :, :, inner_peer(d)], first_a.at[c, d - 1],
                              rs_send.at[0, c, d - 1], rs_recv.at[0, c, d - 1], at(jy, inner_peer(d)))
                       for d in steps_in])
        rs1[1].append([remote(part.at[pb, :, outer_peer(e)], first_b.at[c, e - 1],
                              rs_send.at[1, c, e - 1], rs_recv.at[1, c, e - 1], at(outer_peer(e), ix))
                       for e in steps_out])
        rs2[0].append([remote(mid_a.at[c, e - 1], second_a.at[c, e - 1],
                              rs_send.at[2, c, e - 1], rs_recv.at[2, c, e - 1], at(outer_peer(e), ix))
                       for e in steps_out])
        rs2[1].append([remote(mid_b.at[c, d - 1], second_b.at[c, d - 1],
                              rs_send.at[3, c, d - 1], rs_recv.at[3, c, d - 1], at(jy, inner_peer(d)))
                       for d in steps_in])

    n_first = (inner - 1) * outer + (outer - 1) * inner
    for copy in loads[:n_first]:
        copy.wait()
    for c in range(CHUNKS):
        for d, copy in zip(steps_in, rs1[0][c]):
            sums_over(outer, lambda n: (c, outer_peer(n), inner_peer(d)))
            copy.start()
        for e, copy in zip(steps_out, rs1[1][c]):
            sums_over(inner, lambda n: (CHUNKS + c, outer_peer(e), inner_peer(n)))
            copy.start()
    for copy in loads[n_first:]:
        copy.wait()
    sums_over(CHUNKS * outer, lambda n: (n // outer, n % outer, ix))
    sums_over(CHUNKS * inner, lambda n: (CHUNKS + n // inner, jy, n % inner))

    for c in range(CHUNKS):
        for copy in rs1[0][c]:
            copy.wait_recv()
        for e, copy in zip(steps_out, rs2[0][c]):
            total = part[c, :, outer_peer(e), ix]
            for d in steps_in:
                total = total + first_a[c, d - 1, :, outer_peer(e)]
            mid_a[c, e - 1] = total
            copy.start()
        for copy in rs1[1][c]:
            copy.wait_recv()
        for d, copy in zip(steps_in, rs2[1][c]):
            total = part[CHUNKS + c, :, jy, inner_peer(d)]
            for e in steps_out:
                total = total + first_b[c, e - 1, :, inner_peer(d)]
            mid_b[c, d - 1] = total
            copy.start()

    def gathers(unit, row0, p):
        sends, relays = [], []

        def move(j, i, to, sem):
            ref = ext.at[pl.ds(unit, slots) if unit else pl.ds(0, 1), j, i, p]
            return remote(ref, ref, ag_send.at[row0, p, sem], ag_recv.at[row0, p, sem], to)

        sem = 0
        for d in steps_in:
            sends.append(("in", d, move(jy, ix, at(jy, inner_peer(d)), sem)))
            sem += 1
        for e in steps_out:
            sends.append(("out", e, move(jy, ix, at(outer_peer(e), ix), sem)))
            sem += 1
        if row0 in DIRECT:
            for d in steps_in:
                for e in steps_out:
                    sends.append(("diagonal", d, move(jy, ix, at(outer_peer(e), inner_peer(d)), sem)))
                    sem += 1
        elif p < CHUNKS:
            for d in steps_in:
                for e in steps_out:
                    relays.append((d, move(jy, inner_peer(inner - d), at(outer_peer(e), ix), sem)))
                    sem += 1
        else:
            for e in steps_out:
                for d in steps_in:
                    relays.append((e, move(outer_peer(outer - e), ix, at(jy, inner_peer(d)), sem)))
                    sem += 1
        return sends, relays

    parts = range(2 * CHUNKS)
    turn = [o * CHUNKS + c for c in range(CHUNKS) for o in range(2)]
    slot_gathers = [gathers(1, 0, p) for p in parts]
    early_gathers = [gathers(0, 1, p) for p in parts]

    def start_gather(g):
        for _, _, copy in g[0]:
            copy.start()

    def relay_gather(g, p):
        kind = "in" if p < CHUNKS else "out"
        for name, d, copy in g[0]:
            if name == kind:
                copy.wait_recv()
                for dd, forward in g[1]:
                    if dd == d:
                        forward.start()

    def finish_gather(g, p):
        kind = "in" if p < CHUNKS else "out"
        for name, _, copy in g[0]:
            if name != kind:
                copy.wait_recv()
        for _, forward in g[1]:
            forward.wait_recv()
        for _, _, copy in g[0]:
            copy.wait_send()
        for _, forward in g[1]:
            forward.wait_send()

    chain = [remote(passing.at[p], ext.at[0, jy, ix, p], z_send.at[p], z_recv.at[p], {"tm": tm + 1})
             for p in parts]

    def add_slots(p):
        total = ext[1, jy, ix, p]
        for t in range(1, slots):
            total = total + ext[1 + t, jy, ix, p]
        return total

    def own_total(p):
        c = p % CHUNKS
        total = part[p, :, jy, ix]
        if p < CHUNKS:
            for d in steps_in:
                total = total + first_a[c, d - 1, :, jy]
            for copy in rs2[0][c]:
                copy.wait_recv()
            for e in steps_out:
                total = total + second_a[c, e - 1]
        else:
            for e in steps_out:
                total = total + first_b[c, e - 1, :, ix]
            for copy in rs2[1][c]:
                copy.wait_recv()
            for d in steps_in:
                total = total + second_b[c, d - 1]
        ext[pl.ds(1, slots), jy, ix, p] = total

    for p in turn:
        own_total(p)

        @pl.when(tm == 0)
        def _():
            ext[0, jy, ix, p] = jnp.zeros(ext.shape[4:], jnp.float32)
            if steps_tm > 1:
                passing[p] = add_slots(p)
                chain[p].start()

        start_gather(slot_gathers[p])

    def earlier(p):
        @pl.when(tm > 0)
        def _():
            chain[p].wait_recv()

            @pl.when(tm < steps_tm - 1)
            def _():
                passing[p] = ext[0, jy, ix, p] + add_slots(p)
                chain[p].start()

        start_gather(early_gathers[p])

    @pl.when(tm == 1)
    def _():
        for p in turn:
            earlier(p)
            relay_gather(slot_gathers[p], p)

    @pl.when(tm != 1)
    def _():
        for p in turn:
            relay_gather(slot_gathers[p], p)
        for p in turn:
            earlier(p)

    for p in turn:
        relay_gather(early_gathers[p], p)
    for p in turn:
        finish_gather(slot_gathers[p], p)
    for p in turn:
        finish_gather(early_gathers[p], p)

    @pl.when(tm < steps_tm - 1)
    def _():
        for p in parts:
            chain[p].wait_send()

    for copy in halos:
        copy.wait_send()
    for group in rs1 + rs2:
        for copies in group:
            for copy in copies:
                copy.wait_send()


def blend(slots, ext, index, weight, out, held, sems):
    windows, total_rows, _ = out.shape
    size = total_rows // PIECES
    local = [index[w] - lax.axis_index("tm") * slots for w in range(windows)]
    shares = [[jnp.where(local[w] > t, 1.0, jnp.where(local[w] == t, weight[w], 0.0))
               for t in range(slots)] for w in range(windows)]
    copies = []
    for n in range(PIECES):
        span = pl.ds(n * size, size)
        for w in range(windows):
            total = ext[0, span]
            for t in range(slots):
                total = total + shares[w][t] * ext[1 + t, span]
            held[w, span] = total
        copy = pltpu.make_async_copy(held.at[:, span], out.at[:, span], sems.at[n])
        copy.start()
        copies.append(copy)
    for copy in copies:
        copy.wait()


def rows_view(x, nx, gy):
    lead = x.shape[:-2]
    x = x.reshape(lead + (nx, gy // LANES, LANES))
    x = jnp.swapaxes(x, -3, -2)
    return x


def per_device(control, vertical_modes, mode_counts, perturbations, slot_index, blend_weight):
    members, slots, levels, nx, gy = perturbations.shape
    modes_n = control.shape[1]
    halves = gy // LANES
    level_rows = nx * halves
    tiles, n_mem, steps_tm = lax.axis_size("tile"), lax.axis_size("mem"), lax.axis_size("tm")
    inner = 2 if n_mem % 2 == 0 else 1
    outer = n_mem // inner
    parts = 2 * CHUNKS
    rows = levels // (n_mem * parts) * level_rows
    assert nx >= SMOOTH and level_rows == 8 and rows % 16 == 0
    norm = 1.0 / math.sqrt(members * n_mem - 1)
    fields = members * modes_n
    c = rows_view(control, nx, gy).reshape(fields, level_rows, LANES)
    q = rows_view(perturbations, nx, gy).reshape(members, slots, outer, inner, parts, rows, LANES)
    dims = (members, slots, modes_n, nx, halves, outer, inner, rows, tiles, steps_tm, norm)
    f32 = jnp.float32
    n_in, n_out = max(inner - 1, 1), max(outer - 1, 1)
    n_gather = max(inner - 1 + outer - 1 + (inner - 1) * (outer - 1), 1)
    dma = pltpu.SemaphoreType.DMA
    ext = pl.pallas_call(
        functools.partial(kernel, dims),
        out_shape=pltpu.VMEM((slots + 1, outer, inner, parts, rows, LANES), f32),
        in_specs=[
            pl.BlockSpec(memory_space=pltpu.HBM),
            pl.BlockSpec(memory_space=pltpu.HBM),
            pl.BlockSpec(memory_space=pltpu.SMEM),
            pl.BlockSpec(memory_space=pltpu.SMEM),
        ],
        out_specs=pl.BlockSpec(memory_space=pltpu.VMEM),
        scratch_shapes=[
            pltpu.VMEM((fields, level_rows, LANES), f32),
            pltpu.VMEM((2, fields, level_rows, LANES), f32),
            pltpu.VMEM(q.shape, q.dtype),
            pltpu.VMEM((fields, level_rows, LANES), f32),
            pltpu.VMEM((parts, slots, outer, inner, rows, LANES), f32),
            pltpu.VMEM((CHUNKS, n_in, slots, outer, rows, LANES), f32),
            pltpu.VMEM((CHUNKS, n_out, slots, inner, rows, LANES), f32),
            pltpu.VMEM((CHUNKS, n_out, slots, rows, LANES), f32),
            pltpu.VMEM((CHUNKS, n_in, slots, rows, LANES), f32),
            pltpu.VMEM((CHUNKS, n_out, slots, rows, LANES), f32),
            pltpu.VMEM((CHUNKS, n_in, slots, rows, LANES), f32),
            pltpu.VMEM((parts, rows, LANES), f32),
            dma,
            dma((2 * n_mem,)),
            dma((2,)),
            dma((2,)),
            dma((4, CHUNKS, max(n_in, n_out))),
            dma((4, CHUNKS, max(n_in, n_out))),
            dma((parts,)),
            dma((parts,)),
            dma((2, parts, n_gather)),
            dma((2, parts, n_gather)),
        ],
        compiler_params=pltpu.CompilerParams(
            collective_id=0, has_side_effects=True),
    )(c, q, vertical_modes.T, mode_counts)
    ext = ext.reshape(slots + 1, levels * level_rows, LANES)
    windows = slot_index.shape[0]
    out = pl.pallas_call(
        functools.partial(blend, slots),
        out_shape=jax.ShapeDtypeStruct((windows, levels * level_rows, LANES), f32),
        in_specs=[
            pl.BlockSpec(memory_space=pltpu.VMEM),
            pl.BlockSpec(memory_space=pltpu.SMEM),
            pl.BlockSpec(memory_space=pltpu.SMEM),
        ],
        out_specs=pl.BlockSpec(memory_space=pltpu.HBM),
        scratch_shapes=[pltpu.VMEM((windows, levels * level_rows, LANES), f32), dma((PIECES,))],
        compiler_params=pltpu.CompilerParams(vmem_limit_bytes=8 << 20),
    )(ext, slot_index, blend_weight)
    out = out.reshape(windows, levels, halves, nx, LANES)
    return jnp.swapaxes(out, 2, 3).reshape(windows, levels, nx, gy)


def solution(mesh):
    placed = (
        P("mem", None, "tile", None),
        P(),
        P("tile"),
        P("mem", "tm", None, "tile", None),
        P("tm"),
        P("tm"),
    )
    return jax.shard_map(
        per_device,
        mesh=mesh,
        in_specs=placed,
        out_specs=P("tm", None, "tile", None),
        check_vma=False,
    )
```
